1024 devices in a mesh: dp: 32 (over y, x, core), expert: 32 (over z).
Axes of the slice: x: 4, y: 4, z: 32, core: 2. Of those that a mesh axis runs over, the one named last changes fastest.
Arguments:
- tokens_in: bfloat16 [131072, 2048], P(('dp', 'expert')), may hold values from -6 to 6
- out_grad: bfloat16 [131072, 2048], P(('dp', 'expert')), may hold values from -3 to 3
- expert_ids: int32 [131072, 8], P(('dp', 'expert')), may hold values from 0 to 127, all different within a row; in each aligned block of 128 rows (0 to 127, 128 to 255, ...) at most 16 rows name the same one
- rest_scores: float32 [131072, 8], P(('dp', 'expert')), may hold values from -60 to 60
- router_weight: bfloat16 [2048, 128], replicated, may hold values from -0.125 to 0.125
- down_weight: bfloat16 [32, 768, 2048], P('expert'), may hold values from -0.125 to 0.125
- saved_hidden: bfloat16 [32, 32, 32, 16, 768], P('dp', 'expert'), may hold values from -6 to 6
Outputs:
- token_grad: bfloat16 [131072, 2048], P(('dp', 'expert'))
- router_grad: float32 [2048, 128], P('dp', 'expert')
- down_grad: float32 [32, 768, 2048], P('expert', 'dp')
- hidden_grad: bfloat16 [32, 32, 32, 16, 768], P('dp', 'expert')
The draws below stay inside these ranges and needn't reach their ends.
Inputs may be any that keep to these rules, and one draw needn't show every extreme that they name: `expert_ids`: each row names 8 different experts; among the 128 tokens of one device no expert is named more than 16 times, a bound that some block reaches.
All inputs are finite; a program needn't handle non-finite values.
Results may differ from the reference program's by a relative error of at most 0.024.
Values may be sent and summed in bfloat16 or wider, within the bound.
No kernel may reach another device: no remote copies, remote signals or barrier semaphores. Data moves between devices by JAX's collectives and lax.ppermute only.
A program may use at most 64 MiB of HBM per device.

```python
import math
import jax
import jax.numpy as jnp
import numpy as np
from jax import lax

D = 2048
FF = 768
EXPERTS = 128
TOPK = 8
TOK_DEV = 128
CAP = 16
WIN = 32
TOKENS = 131072
N_DP = 32
N_EXPERT = 32


def level_of(stream_key, shape, split, low, top_value):
    factor_of = 1.0
    for axis_at, blocks in split:
        steps = jax.random.uniform(jax.random.fold_in(jax.random.fold_in(stream_key, 6), axis_at), (blocks,), jnp.float32, low / len(split), top_value / len(split))
        factor_of = factor_of * jnp.repeat(jnp.exp(steps), shape[axis_at] // blocks).reshape((-1,) + (1,) * (len(shape) - 1 - axis_at))
    return factor_of


def routed_block(key, own, number, rows, count, top, limit, lean):
    order = jax.random.permutation(key, count)
    crowded, usual = shares(count, rows * top, limit, lean, True), shares(count, rows * top, limit, lean, False)
    places = jnp.arange(count)

    def named(sizes, offset_by):
        used = int((sizes > 0).sum())
        fixed = max(1, used // 4)
        passed = fixed + (places - fixed + offset_by * (used - fixed)) % max(1, count - fixed)
        return jnp.zeros((count,), jnp.int32).at[order[jnp.where(places < fixed, places, passed)]].set(jnp.asarray(sizes, jnp.int32))

    sizes = jnp.where(number % 4 == 0, named(crowded, number // 4), named(usual, number - number // 4 - 1))
    mixed = jax.random.permutation(jax.random.fold_in(own, 3), count)
    source_of, sink = mixed[0:count // 2 * 2:2], mixed[1:count // 2 * 2:2]
    room = jnp.minimum(sizes[source_of] - 1, limit - sizes[sink]) // 2
    room = jnp.where((source_of == order[0]) | (sink == order[0]) | (sizes[sink] == 0), 0, jnp.maximum(room, 0))
    passed = jax.random.randint(jax.random.fold_in(own, 4), (count // 2,), 0, 1 << 20) % (room + 1)
    sizes = sizes.at[source_of].add(-passed).at[sink].add(passed)
    items = jnp.searchsorted(jnp.cumsum(sizes), jnp.arange(rows * top), side="right").astype(jnp.int32)
    grid = items.reshape(top, rows).T
    grid = grid[jax.random.permutation(jax.random.fold_in(own, 1), rows)]
    offset_by = jax.random.randint(jax.random.fold_in(own, 2), (rows, 1), 0, top)
    return jnp.take_along_axis(grid, (jnp.arange(top)[None, :] + offset_by) % top, axis=1)


def shares(number_of, total, bound, slope, full):
    portions = [(1 << 20) // math.isqrt(grade ** slope) + 1 for grade in range(1, number_of + 1)]
    largest = bound if full else min(bound, max(-(-total // number_of), total * portions[0] // sum(portions)))
    least = 1 if total - largest >= number_of - 1 else 0
    holding, rest = [largest] + [least] * (number_of - 1), total - largest - least * (number_of - 1)
    while rest > 0:
        free = [i for i in range(1, number_of) if holding[i] < largest] or [i for i in range(1, number_of) if holding[i] < bound]
        pool, remaining = sum([portions[i] for i in free]), rest
        for i in free:
            addition = min(bound - holding[i], max(1, remaining * portions[i] // pool), rest)
            holding[i] = holding[i] + addition
            rest = rest - addition
    return np.array(holding)


def bell_draw(own_key, shape, scale, limit, shards=(), kind=jnp.bfloat16):
    entries = jax.random.normal(own_key, shape, jnp.float32) * scale
    if len(shards) > 0:
        entries = level_of(own_key, shape, shards, -0.22, 0.18) * entries
    return jnp.clip(entries, min=-limit, max=limit).astype(kind)


def setup_inputs(seed: int = 0) -> dict:
    streams_of = jax.random.split(jax.random.key(seed), 8)
    tokens_in = bell_draw(streams_of[0], (TOKENS, D), 1.0, 6.0, ((0, 1024),))
    out_grad = bell_draw(streams_of[1], (TOKENS, D), 0.5, 3.0, ((0, 1024),))
    expert_ids_keys = jax.random.split(jax.random.fold_in(streams_of[2], 1), TOKENS // TOK_DEV)
    expert_ids_turns = jax.random.permutation(jax.random.fold_in(streams_of[2], 3), TOKENS // TOK_DEV)
    expert_ids = jax.vmap(lambda own, number: routed_block(jax.random.fold_in(streams_of[2], 2), own, number, TOK_DEV, EXPERTS, TOPK, CAP, 2))(expert_ids_keys, expert_ids_turns).reshape((TOKENS, TOPK))
    rest_scores = bell_draw(streams_of[3], (TOKENS, TOPK), 10.0, 60.0, ((0, 1024),), jnp.float32)
    router_weight = bell_draw(streams_of[4], (D, EXPERTS), D ** -0.5, 0.125)
    down_weight = bell_draw(streams_of[5], (WIN, FF, D), D ** -0.5, 0.125, ((0, 32),))
    saved_hidden = bell_draw(streams_of[6], (N_DP, WIN, N_EXPERT, CAP, FF), 1.0, 6.0, ((0, 32), (1, 32)))
    return {"tokens_in": tokens_in, "out_grad": out_grad, "expert_ids": expert_ids, "rest_scores": rest_scores, "router_weight": router_weight, "down_weight": down_weight, "saved_hidden": saved_hidden}


def slot_layout(ids_block, window, capacity):
    hit_mask = (ids_block[:, :, None] == jnp.arange(window, dtype=jnp.int32)[None, None, :]).astype(jnp.int32)
    chosen = jnp.sum(hit_mask, axis=1)
    before = jnp.cumsum(chosen, axis=0) - chosen
    placed = (chosen[None, :, :] == 1) & (before[None, :, :] == jnp.arange(capacity, dtype=jnp.int32)[:, None, None])
    slot_table = jnp.transpose(placed, (2, 0, 1)).astype(jnp.float32)
    return slot_table, hit_mask.astype(jnp.float32)


def reference(tokens_in, out_grad, expert_ids, rest_scores, router_weight, down_weight, saved_hidden):
    window = N_EXPERT
    capacity = saved_hidden.shape[3]
    sources = N_EXPERT
    logits = jnp.dot(tokens_in, router_weight, preferred_element_type=jnp.float32)
    picked = jnp.take_along_axis(logits, expert_ids, axis=1)
    gate_sel = jax.nn.softmax(picked, axis=1)
    grad_rows = out_grad.reshape(N_DP, sources, TOK_DEV, D)
    ids_rows = expert_ids.reshape(N_DP, sources, TOK_DEV, TOPK)
    gate_rows = gate_sel.reshape(N_DP, sources, TOK_DEV, TOPK)
    weight_f = down_weight.astype(jnp.float32)

    def one_row(total, packed):
        grad_blk, ids_blk, gate_blk, hidden_blk = packed
        slot_table, hit_mask = jax.vmap(lambda ids: slot_layout(ids, window, capacity))(ids_blk)
        gate_each = jnp.einsum('stkw,stk->stw', hit_mask, gate_blk)
        position = jnp.sum(slot_table * jnp.arange(TOK_DEV, dtype=jnp.float32), axis=-1).astype(jnp.int32)
        filled = jnp.sum(slot_table, axis=-1)
        sent_grad = jax.vmap(lambda grads, where_at: grads[where_at])(grad_blk, position)
        sent_grad = sent_grad * filled[..., None].astype(jnp.bfloat16)
        sent_gate = jnp.einsum('swct,stw->swc', slot_table, gate_each).astype(jnp.bfloat16)
        got_grad = jnp.transpose(sent_grad, (1, 0, 2, 3)).astype(jnp.float32)
        got_gate = jnp.transpose(sent_gate, (1, 0, 2)).astype(jnp.float32)
        raw_grad = jnp.einsum('wscd,wfd->wscf', got_grad, weight_f)
        hidden_f = hidden_blk.astype(jnp.float32)
        hid_grad = (got_gate[..., None] * raw_grad).astype(jnp.bfloat16)
        scores = jnp.sum(raw_grad * hidden_f, axis=-1)
        scaled = lax.optimization_barrier((got_gate[..., None] * got_grad).astype(jnp.bfloat16)).astype(jnp.float32)
        partial_value = jnp.einsum('wscf,wscd->wfd', hidden_f, scaled)
        partial_value = lax.optimization_barrier(partial_value.astype(jnp.bfloat16)).astype(jnp.float32)
        per_token = jnp.einsum('swct,wsc->stw', slot_table, scores)
        score_tok = jnp.einsum('stkw,stw->stk', hit_mask, per_token)
        return total + partial_value, (hid_grad, score_tok)

    start_total = jnp.zeros((window, FF, D), jnp.float32)
    down_grad, (hidden_grad, score_rows) = lax.scan(one_row, start_total, (grad_rows, ids_rows, gate_rows, saved_hidden))
    score_all = score_rows.reshape(TOKENS, TOPK)
    score_all = jnp.where(expert_ids < window, score_all, rest_scores)
    mean_part = jnp.sum(gate_sel * score_all, axis=1, keepdims=True)
    logit_sel = gate_sel * (score_all - mean_part)
    row_index = jnp.arange(TOKENS, dtype=jnp.int32)[:, None]
    logit_grad = jnp.zeros((TOKENS, EXPERTS), jnp.float32).at[row_index, expert_ids].add(logit_sel)
    logit_bf = logit_grad.astype(jnp.bfloat16)
    router_grad = jnp.dot(tokens_in.T, logit_bf, preferred_element_type=jnp.float32)
    token_grad = jnp.dot(logit_bf, router_weight.T, preferred_element_type=jnp.float32).astype(jnp.bfloat16)
    return token_grad, router_grad, down_grad, hidden_grad
```

```python
import jax
import jax.numpy as jnp
from jax import lax
from jax.sharding import PartitionSpec as P


F32 = jnp.float32
BF16 = jnp.bfloat16
NEAR = 8


def in_blocks(value, dim, peers):
    before, after = (value.shape[:dim], value.shape[dim + 1 :])
    return jnp.moveaxis(value.reshape(*before, peers, -1, *after), dim, 0)


def sum_at_owner(value, axis, dim):
    parts = in_blocks(value, dim, lax.axis_size(axis))
    arrived = lax.all_to_all(parts, axis, split_axis=0, concat_axis=0, tiled=True)
    return arrived.astype(F32).sum(axis=0)


def turned(value, start):
    twice = jnp.concatenate([value, value], axis=0)
    return lax.dynamic_slice_in_dim(twice, start, value.shape[0], axis=0)


def shift(value, step):
    n = lax.axis_size("expert")
    return lax.ppermute(value, "expert", [(k, (k + step) % n) for k in range(n)])


def shift_by_core(value, step):
    rows, n = lax.axis_size("dp"), lax.axis_size("expert")
    pairs = []
    for i in range(rows):
        way = step if i % 2 == 0 else -step
        pairs += [(i * n + k, i * n + (k + way) % n) for k in range(n)]
    return lax.ppermute(value, ("dp", "expert"), pairs)


def picker(places, gates, tokens):
    at = lax.broadcasted_iota(jnp.int32, (*places.shape, tokens), places.ndim)
    hit = at == places.astype(jnp.int32)[..., None]
    return jnp.where(hit, gates[..., None], 0.0).astype(BF16)


def pick(table, rows):
    return lax.dot_general(
        table, rows, (((1,), (0,)), ((), ())), preferred_element_type=F32
    ).astype(BF16)


def through(rows, weight, hidden):
    raw = lax.dot_general(rows, weight, (((1,), (1,)), ((), ())), preferred_element_type=F32)
    return raw.astype(BF16), jnp.sum(raw * hidden.astype(F32), axis=1)


def across(hidden, rows):
    return lax.dot_general(hidden, rows, (((0,), (0,)), ((), ())), preferred_element_type=F32)


SIDE = 4


def from_peers(parts, mine, place, perm_of, count):
    total = lax.dynamic_index_in_dim(parts, mine, 0, keepdims=False).astype(F32)
    for step in range(1, count):
        out = lax.dynamic_index_in_dim(parts, (mine + step) % count, 0, keepdims=False)
        got = lax.ppermute(out, "dp", [(i, perm_of(i, step)) for i in range(place)])
        total = total + got.astype(F32)
    return total


def sum_over_cores(partial):
    size = lax.axis_size("dp")
    width = partial.shape[1]
    core = lax.axis_index("dp") % 2
    parts = jnp.moveaxis(partial.reshape(size // 2, 2, -1, width), 1, 0)
    return from_peers(parts, core, size, lambda i, step: i ^ 1, 2).astype(BF16)


def sum_over_chips(halves):
    size = lax.axis_size("dp")
    at = lax.axis_index("dp") // 2
    rows, width = halves.shape[1:]
    sides = size // 2 // SIDE

    def in_x(i, step):
        return (i // (2 * SIDE)) * 2 * SIDE + ((i // 2 % SIDE + step) % SIDE) * 2 + i % 2

    def in_y(i, step):
        return ((i // (2 * SIDE) + step) % sides) * 2 * SIDE + i % (2 * SIDE)

    by_x = jnp.moveaxis(halves.reshape(sides, SIDE, rows, width), 1, 0)
    row = from_peers(by_x, at % SIDE, size, in_x, SIDE).astype(BF16)
    return from_peers(row, at // SIDE, size, in_y, sides)


def shards(tokens_in, out_grad, expert_ids, rest_scores, router_weight, down_weight, saved_hidden):
    n = lax.axis_size("expert")
    me = lax.axis_index("expert")
    even = lax.axis_index("dp") % 2 == 0
    capacity = saved_hidden.shape[3]
    hidden_units = saved_hidden.shape[4]
    tokens, width = out_grad.shape
    scored = router_weight.shape[1]
    top = expert_ids.shape[1]

    up, down = [out_grad], [out_grad]
    for _ in range(1, NEAR + 1):
        up.append(shift(up[-1], 1))
        down.append(shift(down[-1], -1))

    ids_t = expert_ids.T
    rest_t = rest_scores.T
    expert_at = lax.broadcasted_iota(jnp.int32, (scored, tokens), 0)
    logits = lax.dot_general(
        router_weight, tokens_in, (((0,), (1,)), ((), ())), preferred_element_type=F32
    )
    chosen = jnp.zeros((scored, tokens), jnp.bool_)
    rest = jnp.zeros((scored, tokens), F32)
    for k in range(top):
        same = expert_at == ids_t[k][None, :]
        chosen = chosen | same
        rest = jnp.where(same, rest_t[k][None, :], rest)
    highest = jnp.max(jnp.where(chosen, logits, -jnp.inf), axis=0, keepdims=True)
    power = jnp.where(chosen, jnp.exp(logits - highest), 0.0)
    gate = power / jnp.sum(power, axis=0, keepdims=True)
    hit = chosen[:n]
    earlier = lax.broadcasted_iota(jnp.int32, (tokens, tokens), 0) < lax.broadcasted_iota(
        jnp.int32, (tokens, tokens), 1
    )
    before = lax.dot_general(
        hit.astype(BF16), earlier.astype(BF16), (((1,), (0,)), ((), ())), preferred_element_type=F32
    )
    slot = jnp.where(hit, before, -1.0)
    gate_sent = gate[:n].astype(BF16).astype(F32)
    token_at = lax.broadcasted_iota(jnp.int32, (n, tokens), 1).astype(F32)
    placed = slot[:, None, :] == jnp.arange(capacity, dtype=F32)[None, :, None]
    place = jnp.sum(jnp.where(placed, token_at[:, None, :], 0.0), axis=2)
    slot_gate = jnp.sum(jnp.where(placed, gate_sent[:, None, :], 0.0), axis=2)
    meta = jnp.concatenate([place, slot_gate], axis=1)
    far_up = turned(meta, (me + NEAR + 1) % n)[:NEAR]
    far_down = turned(meta, (me + n - 2 * NEAR) % n)[:NEAR][::-1]
    last = lax.broadcasted_iota(jnp.int32, far_up.shape, 0) == NEAR - 1
    far_up = jnp.where(last & ~even, 0.0, far_up)
    far_down = jnp.where(last & even, 0.0, far_down)
    peer = jnp.arange(n)[:, None, None]
    far = jnp.where(peer == (me + NEAR) % n, far_up[None], 0.0) + jnp.where(
        peer == (me + n - NEAR) % n, far_down[None], 0.0
    )
    note = jnp.concatenate([meta[:, None], far], axis=1).reshape(n, 1, -1)
    note = lax.all_to_all(note, "expert", split_axis=0, concat_axis=0, tiled=True)
    note = turned(note, me)
    note = note.reshape(n, NEAR + 1, 2, capacity)

    back = [(n - h) % n for h in range(NEAR + 1)]
    far_up_rows = pick(
        picker(note[back[NEAR], 1:, 0], note[back[NEAR], 1:, 1], tokens).reshape(-1, tokens), up[NEAR]
    ).reshape(NEAR, capacity, width)
    far_down_rows = pick(
        picker(note[NEAR, 1:, 0], note[NEAR, 1:, 1], tokens).reshape(-1, tokens), down[NEAR]
    ).reshape(NEAR, capacity, width)
    opposite = shift_by_core(jnp.where(even, far_up_rows[-1], far_down_rows[-1]), NEAR)
    far_from_below, far_from_above = {}, {}
    for j in range(NEAR - 1, 0, -1):
        far_from_below[j] = shift(far_up_rows[j - 1], j)
        far_from_above[j] = shift(far_down_rows[j - 1], -j)

    near_table = picker(note[:, 0, 0], note[:, 0, 1], tokens)
    near_rows = [pick(near_table[n - h], up[h]) for h in range(NEAR, 0, -1)]
    near_rows += [pick(near_table[h], down[h]) for h in range(NEAR + 1)]
    far_rows = [far_from_above[j] for j in range(1, NEAR)] + [opposite]
    far_rows += [far_from_below[j] for j in range(NEAR - 1, 0, -1)]
    near = jnp.concatenate(near_rows, axis=0)
    far = jnp.concatenate(far_rows, axis=0)
    cut = near.shape[0]

    hidden = turned(saved_hidden[0, 0], (me + n - NEAR) % n).reshape(n * capacity, hidden_units)
    hid_near, score_near = through(near, down_weight[0], hidden[:cut])
    far, score_near = lax.optimization_barrier((far, score_near))
    hid_far, score_far = through(far, down_weight[0], hidden[cut:])
    home = (NEAR + n - me) % n
    scores = jnp.concatenate([score_near, score_far], axis=0).reshape(n, 1, capacity)
    scores, far = lax.optimization_barrier((turned(scores, home), far))
    returned = lax.all_to_all(scores, "expert", split_axis=0, concat_axis=0, tiled=True)[:, 0]
    partial = (across(hidden[:cut], near) + across(hidden[cut:], far)).astype(BF16)
    halves = sum_over_cores(partial)
    down_grad = sum_over_chips(halves)
    hid_grad = jnp.concatenate([hid_near, hid_far], axis=0)
    hidden_grad = turned(hid_grad.reshape(n, capacity, hidden_units), home)

    there = jnp.sum(jnp.where(placed, returned[:, :, None], 0.0), axis=1)
    safe = jnp.where(gate_sent > 0.0, gate_sent, 1.0)
    there = jnp.where(gate_sent > 0.0, there * (gate[:n] / safe), 0.0)
    weighed = jnp.concatenate([there, (gate * rest)[n:]], axis=0)
    logit_grad = (weighed - gate * jnp.sum(weighed, axis=0, keepdims=True)).astype(BF16)
    share = lax.dot_general(
        tokens_in, logit_grad, (((0,), (1,)), ((), ())), preferred_element_type=F32
    ).astype(BF16)
    summed_rows = sum_at_owner(share, "dp", 0)
    router_grad = sum_at_owner(summed_rows.astype(BF16), "expert", 1)
    token_grad = lax.dot_general(
        logit_grad, router_weight, (((0,), (1,)), ((), ())), preferred_element_type=F32
    ).astype(BF16)
    return (token_grad, router_grad, down_grad[None], hidden_grad[None, None])


def solution(mesh):
    return jax.shard_map(
        shards,
        mesh=mesh,
        in_specs=(
            P(("dp", "expert"), None),
            P(("dp", "expert"), None),
            P(("dp", "expert"), None),
            P(("dp", "expert"), None),
            P(),
            P("expert", None, None),
            P("dp", "expert", None, None, None),
        ),
        out_specs=(
            P(("dp", "expert"), None),
            P("dp", "expert"),
            P("expert", "dp", None),
            P("dp", "expert", None, None, None),
        ),
        check_vma=False,
    )
```

```python
import jax
import jax.numpy as jnp
import numpy as np
from jax import lax
from jax.sharding import PartitionSpec as P


F32 = jnp.float32
BF16 = jnp.bfloat16
NEAR = 9
LANES = 128


def in_blocks(value, dim, peers):
    before, after = (value.shape[:dim], value.shape[dim + 1 :])
    return jnp.moveaxis(value.reshape(*before, peers, -1, *after), dim, 0)


def sum_at_owner(value, axis, dim):
    parts = in_blocks(value, dim, lax.axis_size(axis))
    arrived = lax.all_to_all(parts, axis, split_axis=0, concat_axis=0, tiled=True)
    return arrived.astype(F32).sum(axis=0)


def turned(value, start):
    twice = jnp.concatenate([value, value], axis=0)
    return lax.dynamic_slice_in_dim(twice, start, value.shape[0], axis=0)


def shift(value, step):
    n = lax.axis_size("expert")
    return lax.ppermute(value, "expert", [(k, (k + step) % n) for k in range(n)])


def tables(notes, peers, lanes, capacity):
    wanted = np.repeat(np.array(lanes), capacity)[:, None]
    lane = np.arange(LANES)[None]
    gates = row_products(jnp.asarray(lane == wanted, BF16), notes)
    slots = row_products(jnp.asarray(lane == wanted + peers, BF16), notes)
    at = lax.broadcasted_iota(jnp.int32, slots.shape, 0) % capacity
    return jnp.where(slots == at.astype(F32), gates, 0.0).astype(BF16)


def row_products(a, b):
    return lax.dot_general(a, b, (((1,), (1,)), ((), ())), preferred_element_type=F32)


def pick(table, block, width):
    return lax.dot_general(
        table, block[:, :width], (((1,), (0,)), ((), ())), preferred_element_type=F32
    ).astype(BF16)


def spread(rows, capacity, way):
    parts = {k + 1: [(0, r)] for k, r in enumerate(jnp.split(rows, rows.shape[0] // capacity))}
    step = 4
    while step:
        sent = [(k, far, r) for k in sorted(parts) if k >= step for far, r in parts[k]]
        parts = {k: v for k, v in parts.items() if k < step}
        got = shift(jnp.concatenate([r for _, _, r in sent], axis=0), way * step)
        for (k, far, _), r in zip(sent, jnp.split(got, len(sent))):
            parts.setdefault(k - step, []).append((far + step, r))
        step //= 2
    return [r for _, r in sorted(parts[0], key=lambda pair: pair[0])]


def through(rows, weight, hidden):
    raw = lax.dot_general(rows, weight, (((1,), (1,)), ((), ())), preferred_element_type=F32)
    return raw.astype(BF16), jnp.sum(raw * hidden.astype(F32), axis=1)


def across(hidden, rows):
    return lax.dot_general(hidden, rows, (((0,), (0,)), ((), ())), preferred_element_type=F32)


def shards(tokens_in, out_grad, expert_ids, rest_scores, router_weight, down_weight, saved_hidden):
    n = lax.axis_size("expert")
    me = lax.axis_index("expert")
    capacity = saved_hidden.shape[3]
    hidden_units = saved_hidden.shape[4]
    tokens, width = out_grad.shape
    scored = router_weight.shape[1]

    ids_t = expert_ids.T
    rest_t = rest_scores.T
    expert_at = lax.broadcasted_iota(jnp.int32, (scored, tokens), 0)
    logits = lax.dot_general(
        router_weight, tokens_in, (((0,), (1,)), ((), ())), preferred_element_type=F32
    )
    same = expert_at[None] == ids_t[:, None, :]
    chosen = jnp.any(same, axis=0)
    rest = jnp.sum(jnp.where(same, rest_t[:, None, :], 0.0), axis=0)
    highest = jnp.max(jnp.where(chosen, logits, -jnp.inf), axis=0, keepdims=True)
    power = jnp.where(chosen, jnp.exp(logits - highest), 0.0)
    gate = power / jnp.sum(power, axis=0, keepdims=True)
    hit = chosen[:n]
    earlier = lax.broadcasted_iota(jnp.int32, (tokens, tokens), 0) < lax.broadcasted_iota(
        jnp.int32, (tokens, tokens), 1
    )
    before = lax.dot_general(
        hit.astype(BF16), earlier.astype(BF16), (((1,), (0,)), ((), ())), preferred_element_type=F32
    )
    slot = jnp.where(hit, before, -1.0)
    gate_sent = gate[:n].astype(BF16).astype(F32)
    notes = turned(jnp.concatenate([gate_sent, slot], axis=1), me)
    notes = jnp.concatenate([notes[:, :tokens], notes[:, tokens:]], axis=0).T.astype(BF16)
    notes = jnp.pad(notes, ((0, 0), (0, LANES - 2 * n)))
    own = jnp.concatenate([out_grad, notes], axis=1)

    up, down = [own], [own]
    for _ in range(1, NEAR + 1):
        up.append(shift(up[-1], 1))
        down.append(shift(down[-1], -1))

    far_up = list(range(NEAR + 1, n // 2 + 1))
    far_down = [n - k for k in far_up[:-1]]
    up_rows = pick(tables(up[NEAR][:, width:], n, far_up, capacity), up[NEAR], width)
    low_rows = pick(tables(down[NEAR][:, width:], n, far_down, capacity), down[NEAR], width)
    top = spread(up_rows, capacity, 1)
    low = spread(low_rows, capacity, -1)

    blocks = [(h, up[h]) for h in range(NEAR, 0, -1)] + [(0, own)]
    blocks += [(n - h, down[h]) for h in range(1, NEAR + 1)]
    lane = lax.broadcasted_iota(jnp.int32, (tokens, LANES), 1) % n
    mixed = own[:, width:]
    for k, block in blocks:
        mixed = jnp.where(lane == k, block[:, width:], mixed)
    near_table = tables(mixed, n, [k for k, _ in blocks], capacity)
    near_rows = [
        pick(near_table[i * capacity : (i + 1) * capacity], block, width)
        for i, (_, block) in enumerate(blocks)
    ]
    near = jnp.concatenate(near_rows, axis=0)
    far = jnp.concatenate(low + top[::-1], axis=0)
    cut = near.shape[0]

    hidden = turned(saved_hidden[0, 0], (me + n - NEAR) % n).reshape(n * capacity, hidden_units)
    hid_near, score_near = through(near, down_weight[0], hidden[:cut])
    hid_far, score_far = through(far, down_weight[0], hidden[cut:])
    home = (NEAR + n - me) % n
    scores = jnp.concatenate([score_near, score_far], axis=0).reshape(n, 1, capacity)
    scores, far = lax.optimization_barrier((turned(scores, home), far))
    returned = lax.all_to_all(scores, "expert", split_axis=0, concat_axis=0, tiled=True)[:, 0]
    partial = (across(hidden[:cut], near) + across(hidden[cut:], far)).astype(BF16)
    down_grad = lax.psum_scatter(partial, "dp", scatter_dimension=0, tiled=True).astype(F32)
    hid_grad = jnp.concatenate([hid_near, hid_far], axis=0)
    hidden_grad = turned(hid_grad.reshape(n, capacity, hidden_units), home)

    placed = slot[:, None, :] == jnp.arange(capacity, dtype=F32)[None, :, None]
    there = jnp.sum(jnp.where(placed, returned[:, :, None], 0.0), axis=1)
    safe = jnp.where(gate_sent > 0.0, gate_sent, 1.0)
    there = jnp.where(gate_sent > 0.0, there * (gate[:n] / safe), 0.0)
    weighed = jnp.concatenate([there, (gate * rest)[n:]], axis=0)
    logit_grad = (weighed - gate * jnp.sum(weighed, axis=0, keepdims=True)).astype(BF16)
    share = lax.dot_general(
        tokens_in, logit_grad, (((0,), (1,)), ((), ())), preferred_element_type=F32
    ).astype(BF16)
    summed_rows = sum_at_owner(share, "dp", 0)
    router_grad = sum_at_owner(summed_rows.astype(BF16), "expert", 1)
    token_grad = lax.dot_general(
        logit_grad, router_weight, (((0,), (1,)), ((), ())), preferred_element_type=F32
    ).astype(BF16)
    return (token_grad, router_grad, down_grad[None], hidden_grad[None, None])


def solution(mesh):
    return jax.shard_map(
        shards,
        mesh=mesh,
        in_specs=(
            P(("dp", "expert"), None),
            P(("dp", "expert"), None),
            P(("dp", "expert"), None),
            P(("dp", "expert"), None),
            P(),
            P("expert", None, None),
            P("dp", "expert", None, None, None),
        ),
        out_specs=(
            P(("dp", "expert"), None),
            P("dp", "expert"),
            P("expert", "dp", None),
            P("dp", "expert", None, None, None),
        ),
        check_vma=False,
    )
```

```python
import jax
import jax.numpy as jnp
import numpy as np
from jax import lax
from jax.sharding import PartitionSpec as P


F32 = jnp.float32
BF16 = jnp.bfloat16
NEAR = 9
LANES = 128


def in_blocks(value, dim, peers):
    before, after = (value.shape[:dim], value.shape[dim + 1 :])
    return jnp.moveaxis(value.reshape(*before, peers, -1, *after), dim, 0)


def sum_at_owner(value, axis, dim):
    parts = in_blocks(value, dim, lax.axis_size(axis))
    arrived = lax.all_to_all(parts, axis, split_axis=0, concat_axis=0, tiled=True)
    return arrived.astype(F32).sum(axis=0)


def turned(value, start):
    twice = jnp.concatenate([value, value], axis=0)
    return lax.dynamic_slice_in_dim(twice, start, value.shape[0], axis=0)


def shift(value, step):
    n = lax.axis_size("expert")
    return lax.ppermute(value, "expert", [(k, (k + step) % n) for k in range(n)])


def tables(notes, peers, lanes, capacity):
    wanted = np.repeat(np.array(lanes), capacity)[:, None]
    lane = np.arange(LANES)[None]
    gates = row_products(jnp.asarray(lane == wanted, BF16), notes)
    slots = row_products(jnp.asarray(lane == wanted + peers, BF16), notes)
    at = lax.broadcasted_iota(jnp.int32, slots.shape, 0) % capacity
    return jnp.where(slots == at.astype(F32), gates, 0.0).astype(BF16)


def row_products(a, b):
    return lax.dot_general(a, b, (((1,), (1,)), ((), ())), preferred_element_type=F32)


def pick(table, block, width):
    return lax.dot_general(
        table, block[:, :width], (((1,), (0,)), ((), ())), preferred_element_type=F32
    ).astype(BF16)


def spread(pick_far, targets, way):
    step = 4
    sent = [(k + 1, 0, None) for k in range(step - 1, len(targets))]
    rows = pick_far(targets[step - 1 :])
    got = shift(rows, way * step)
    rest = jnp.split(pick_far(targets[: step - 1]), step - 1)
    parts = {k + 1: [(0, r)] for k, r in enumerate(rest)}
    while True:
        for (k, far, _), r in zip(sent, jnp.split(got, len(sent))):
            parts.setdefault(k - step, []).append((far + step, r))
        step //= 2
        if not step:
            break
        sent = [(k, far, r) for k in sorted(parts) if k >= step for far, r in parts[k]]
        parts = {k: v for k, v in parts.items() if k < step}
        got = shift(jnp.concatenate([r for _, _, r in sent], axis=0), way * step)
    return [r for _, r in sorted(parts[0], key=lambda pair: pair[0])]


def through(rows, weight, hidden):
    raw = lax.dot_general(rows, weight, (((1,), (1,)), ((), ())), preferred_element_type=F32)
    return raw.astype(BF16), jnp.sum(raw * hidden.astype(F32), axis=1)


def across(hidden, rows):
    return lax.dot_general(hidden, rows, (((0,), (0,)), ((), ())), preferred_element_type=F32)


SIDE = 4


def from_peers(parts, mine, place, perm_of, count):
    total = lax.dynamic_index_in_dim(parts, mine, 0, keepdims=False).astype(F32)
    for step in range(1, count):
        out = lax.dynamic_index_in_dim(parts, (mine + step) % count, 0, keepdims=False)
        got = lax.ppermute(out, "dp", [(i, perm_of(i, step)) for i in range(place)])
        total = total + got.astype(F32)
    return total


def sum_over_cores(partial):
    size = lax.axis_size("dp")
    width = partial.shape[1]
    core = lax.axis_index("dp") % 2
    parts = jnp.moveaxis(partial.reshape(size // 2, 2, -1, width), 1, 0)
    return from_peers(parts, core, size, lambda i, step: i ^ 1, 2).astype(BF16)


def sum_over_chips(halves):
    size = lax.axis_size("dp")
    at = lax.axis_index("dp") // 2
    rows, width = halves.shape[1:]
    sides = size // 2 // SIDE

    def in_x(i, step):
        return (i // (2 * SIDE)) * 2 * SIDE + ((i // 2 % SIDE + step) % SIDE) * 2 + i % 2

    def in_y(i, step):
        return ((i // (2 * SIDE) + step) % sides) * 2 * SIDE + i % (2 * SIDE)

    by_x = jnp.moveaxis(halves.reshape(sides, SIDE, rows, width), 1, 0)
    row = from_peers(by_x, at % SIDE, size, in_x, SIDE).astype(BF16)
    return from_peers(row, at // SIDE, size, in_y, sides)


def shards(tokens_in, out_grad, expert_ids, rest_scores, router_weight, down_weight, saved_hidden):
    n = lax.axis_size("expert")
    me = lax.axis_index("expert")
    capacity = saved_hidden.shape[3]
    hidden_units = saved_hidden.shape[4]
    tokens, width = out_grad.shape
    scored = router_weight.shape[1]

    ids_t = expert_ids.T
    rest_t = rest_scores.T
    expert_at = lax.broadcasted_iota(jnp.int32, (scored, tokens), 0)
    logits = lax.dot_general(
        router_weight, tokens_in, (((0,), (1,)), ((), ())), preferred_element_type=F32
    )
    same = expert_at[None] == ids_t[:, None, :]
    chosen = jnp.any(same, axis=0)
    rest = jnp.sum(jnp.where(same, rest_t[:, None, :], 0.0), axis=0)
    highest = jnp.max(jnp.where(chosen, logits, -jnp.inf), axis=0, keepdims=True)
    power = jnp.where(chosen, jnp.exp(logits - highest), 0.0)
    gate = power / jnp.sum(power, axis=0, keepdims=True)
    hit = chosen[:n]
    earlier = lax.broadcasted_iota(jnp.int32, (tokens, tokens), 0) < lax.broadcasted_iota(
        jnp.int32, (tokens, tokens), 1
    )
    before = lax.dot_general(
        hit.astype(BF16), earlier.astype(BF16), (((1,), (0,)), ((), ())), preferred_element_type=F32
    )
    slot = jnp.where(hit, before, -1.0)
    gate_sent = gate[:n].astype(BF16).astype(F32)
    notes = turned(jnp.concatenate([gate_sent, slot], axis=1), me)
    notes = jnp.concatenate([notes[:, :tokens], notes[:, tokens:]], axis=0).T.astype(BF16)
    notes = jnp.pad(notes, ((0, 0), (0, LANES - 2 * n)))
    own = jnp.concatenate([out_grad, notes], axis=1)

    up, down = [own], [own]
    for _ in range(1, NEAR + 1):
        up.append(shift(up[-1], 1))
        down.append(shift(down[-1], -1))

    far_up = list(range(NEAR + 1, n // 2 + 1))
    far_down = [n - k for k in far_up[:-1]]

    def far_of(block):
        return lambda lanes: pick(tables(block[:, width:], n, lanes, capacity), block, width)

    top = spread(far_of(up[NEAR]), far_up, 1)
    low = spread(far_of(down[NEAR]), far_down, -1)

    blocks = [(h, up[h]) for h in range(NEAR, 0, -1)] + [(0, own)]
    blocks += [(n - h, down[h]) for h in range(1, NEAR + 1)]
    lane = lax.broadcasted_iota(jnp.int32, (tokens, LANES), 1) % n
    mixed = own[:, width:]
    for k, block in blocks:
        mixed = jnp.where(lane == k, block[:, width:], mixed)
    near_table = tables(mixed, n, [k for k, _ in blocks], capacity)
    near_rows = [
        pick(near_table[i * capacity : (i + 1) * capacity], block, width)
        for i, (_, block) in enumerate(blocks)
    ]
    near = jnp.concatenate(near_rows, axis=0)
    far = jnp.concatenate(low + top[::-1], axis=0)
    cut = near.shape[0]

    hidden = turned(saved_hidden[0, 0], (me + n - NEAR) % n).reshape(n * capacity, hidden_units)
    hid_near, score_near = through(near, down_weight[0], hidden[:cut])
    hid_far, score_far = through(far, down_weight[0], hidden[cut:])
    home = (NEAR + n - me) % n
    scores = jnp.concatenate([score_near, score_far], axis=0).reshape(n, 1, capacity)
    scores, far = lax.optimization_barrier((turned(scores, home), far))
    returned = lax.all_to_all(scores, "expert", split_axis=0, concat_axis=0, tiled=True)[:, 0]
    partial = (across(hidden[:cut], near) + across(hidden[cut:], far)).astype(BF16)
    halves = sum_over_cores(partial)
    down_grad = sum_over_chips(halves)
    hid_grad = jnp.concatenate([hid_near, hid_far], axis=0)
    hidden_grad = turned(hid_grad.reshape(n, capacity, hidden_units), home)

    placed = slot[:, None, :] == jnp.arange(capacity, dtype=F32)[None, :, None]
    there = jnp.sum(jnp.where(placed, returned[:, :, None], 0.0), axis=1)
    safe = jnp.where(gate_sent > 0.0, gate_sent, 1.0)
    there = jnp.where(gate_sent > 0.0, there * (gate[:n] / safe), 0.0)
    weighed = jnp.concatenate([there, (gate * rest)[n:]], axis=0)
    logit_grad = (weighed - gate * jnp.sum(weighed, axis=0, keepdims=True)).astype(BF16)
    share = lax.dot_general(
        tokens_in, logit_grad, (((0,), (1,)), ((), ())), preferred_element_type=F32
    ).astype(BF16)
    summed_rows = sum_at_owner(share, "dp", 0)
    router_grad = sum_at_owner(summed_rows.astype(BF16), "expert", 1)
    token_grad = lax.dot_general(
        logit_grad, router_weight, (((0,), (1,)), ((), ())), preferred_element_type=F32
    ).astype(BF16)
    return (token_grad, router_grad, down_grad[None], hidden_grad[None, None])


def solution(mesh):
    return jax.shard_map(
        shards,
        mesh=mesh,
        in_specs=(
            P(("dp", "expert"), None),
            P(("dp", "expert"), None),
            P(("dp", "expert"), None),
            P(("dp", "expert"), None),
            P(),
            P("expert", None, None),
            P("dp", "expert", None, None, None),
        ),
        out_specs=(
            P(("dp", "expert"), None),
            P("dp", "expert"),
            P("expert", "dp", None),
            P("dp", "expert", None, None, None),
        ),
        check_vma=False,
    )
```
